32 devices in a mesh: group: 4 (over y, x), dom: 8 (over z, core).
Axes of the slice: x: 2, y: 2, z: 4, core: 2. Of those that a mesh axis runs over, the one named last changes fastest.
Arguments:
- p_start: float32 [1024, 128], P(('group', 'dom')), may hold values from -60 to 60
- r_start: float32 [1024, 128], P(('group', 'dom')), may hold values from -60 to 60
- diag_shift: float32 [1024, 128], P(('group', 'dom')), may hold values from 0.5 to 2
- shifts: float32 [8], replicated, may hold values from 0.5 to 1.5
- block_values: float32 [1024, 6, 128, 128], P(('group', 'dom')), may hold values from -0.21875 to 0.21875
- block_cols: int32 [1024, 6], P(('group', 'dom')), may hold values from 0 to 95, as said below
- live_slots: int32 [1024], P(('group', 'dom')), may hold values from 2 to 6, as said below
- needed: int32 [32, 4, 16], P(('group', 'dom')), may hold values from 0 to 31
Outputs:
- basis: float32 [17, 1024, 128], P(None, ('group', 'dom'))
- gram: float32 [17, 17], replicated
The draws below stay inside these ranges and needn't reach their ends.
Inputs may be any that keep to these rules, and one draw needn't show every extreme that they name: `block_cols`: slot 0 of block row b is the row itself (b mod 32); a value below 32 names a block row of the same device, a value 32 + k * 16 + h names entry h of the device's list k of needed. Devices with dom index 0 never use list 0 in used slots, devices with the last dom index never list 1. Slots from live_slots on hold values in range but are not used. `live_slots`: the first block row of every device uses all 6 slots. needed[d, k] lists the local block rows that device d reads from its source s_k(d), in the order of its extended field.
All inputs are finite; a program needn't handle non-finite values.
Results may differ from the reference program's by a relative error of at most 0.0001.
Values sent between devices are 32-bit elements; how exact they have to be, the bound alone decides.
A program may use at most 64 MiB of HBM per device.

```python
import math
import jax
import jax.numpy as jnp
from jax import lax

BS = 128
S = 8
NB = 6
BR_DEV = 32
HALO = 16
NBLK = 1024
N_GROUP = 4
N_DOM = 8


def rough_vector(key):
    total = BR_DEV * N_GROUP * N_DOM
    owners = (jnp.arange(total) // BR_DEV).astype(jnp.float32)
    rise = jnp.exp(math.log(3.0) * owners / max(N_GROUP * N_DOM - 1, 1))
    cell = jnp.exp(jax.random.uniform(jax.random.fold_in(key, 1), (total, BS), jnp.float32, 0.0, math.log(10.0)))
    base = jax.random.normal(jax.random.fold_in(key, 2), (total, BS), jnp.float32)
    return base * cell * rise[:, None] * 0.25


def draw_p_start(key, part):
    return rough_vector(jax.random.fold_in(key, 101))


def draw_r_start(key, part):
    return rough_vector(jax.random.fold_in(key, 202))


def block_pattern(key):
    base_key = jax.random.fold_in(key, 303)
    total = BR_DEV * N_GROUP * N_DOM
    block_ids = jnp.arange(total, dtype=jnp.int32)
    dom_ids = block_ids // BR_DEV % N_DOM
    live = jax.random.randint(jax.random.fold_in(base_key, 1), (total,), 2, NB + 1)
    live = jnp.where(block_ids % BR_DEV == 0, NB, live).astype(jnp.int32)
    local_pick = jax.random.randint(jax.random.fold_in(base_key, 2), (total, NB), 0, BR_DEV)
    source_pick = jax.random.randint(jax.random.fold_in(base_key, 3), (total, NB), 0, 4)
    entry_pick = jax.random.randint(jax.random.fold_in(base_key, 4), (total, NB), 0, HALO)
    remote_pick = jax.random.randint(jax.random.fold_in(base_key, 5), (total, NB), 0, 2)
    missing = (source_pick == 0) & (dom_ids[:, None] == 0) | (source_pick == 1) & (dom_ids[:, None] == N_DOM - 1)
    remote = (remote_pick == 1) & jnp.logical_not(missing)
    cols = jnp.where(remote, BR_DEV + source_pick * HALO + entry_pick, local_pick)
    cols = cols.at[:, 0].set(block_ids % BR_DEV)
    return (cols.astype(jnp.int32), live)


def draw_block_cols(key, part):
    return block_pattern(key)[0]


def draw_live_slots(key, part):
    return block_pattern(key)[1]


def place_ends(values, stream_key, smallest, largest):
    longest = values.shape.index(max(values.shape))
    spots = []
    for shift in (0, 1):
        where = [jax.random.randint(jax.random.fold_in(stream_key, axis), (), 0, length) for axis, length in enumerate(values.shape)]
        where[longest] = (where[longest] + shift) % values.shape[longest]
        spots.append(tuple(where))
    return values.at[spots[0]].set(smallest).at[spots[1]].set(largest)


def shard_levels(own_key, extent, cuts, smallest, largest):
    def one(dim, parts):
        steps = jax.random.uniform(jax.random.fold_in(jax.random.fold_in(own_key, 6), dim), (parts,), jnp.float32, smallest / len(cuts), largest / len(cuts))
        return jnp.repeat(jnp.exp(steps), extent[dim] // parts).reshape((-1,) + (1,) * (len(extent) - dim - 1))

    level = one(*cuts[0])
    for cut in cuts[1:]:
        level = level * one(*cut)
    return level


def bell_draw(rng, shape, width, most, cuts=(), kind=jnp.bfloat16):
    array = jax.random.normal(rng, shape, jnp.float32) * width
    if len(cuts) > 0:
        array = shard_levels(rng, shape, cuts, -0.22, 0.18) * array
    return jnp.clip(array, min=-most, max=most).astype(kind)


def setup_inputs(seed: int = 0) -> dict:
    arg_keys = jax.random.split(jax.random.key(seed), 9)
    p_start = draw_p_start(jax.random.fold_in(arg_keys[8], 71), 0)
    r_start = draw_r_start(jax.random.fold_in(arg_keys[8], 71), 0)
    diag_shift = jnp.clip(jnp.exp(math.log(2.0) - 1.3862944 * jax.random.uniform(arg_keys[2], (NBLK, BS), jnp.float32) ** shard_levels(arg_keys[2], (NBLK, BS), ((0, 32),), -0.2, 0.2)), 0.5, 2.0)
    shifts = jnp.clip(jax.random.uniform(arg_keys[3], (S,), jnp.float32, 0.5, 1.5), 0.5, 1.5)
    block_values = bell_draw(arg_keys[4], (NBLK, NB, BS, BS), (NB * BS) ** -0.5, 0.21875, ((0, 32),), jnp.float32)
    block_cols = draw_block_cols(jax.random.fold_in(arg_keys[8], 71), 0)
    live_slots = draw_live_slots(jax.random.fold_in(arg_keys[8], 71), 0)
    needed = place_ends(jax.random.randint(arg_keys[7], (N_GROUP * N_DOM, 4, HALO), 0, BR_DEV), jax.random.fold_in(arg_keys[7], 1), 0, BR_DEV - 1).astype(jnp.int32)
    return dict(p_start=p_start, r_start=r_start, diag_shift=diag_shift, shifts=shifts, block_values=block_values, block_cols=block_cols, live_slots=live_slots, needed=needed)


def reference(p_start, r_start, diag_shift, shifts, block_values, block_cols, live_slots, needed):
    ndev = N_GROUP * N_DOM
    device_ids = jnp.arange(ndev, dtype=jnp.int32)
    group_ids = device_ids // N_DOM
    dom_ids = device_ids % N_DOM
    sources = [
        group_ids * N_DOM + jnp.maximum(dom_ids - 1, 0),
        group_ids * N_DOM + jnp.minimum(dom_ids + 1, N_DOM - 1),
        ((group_ids - 1) % N_GROUP) * N_DOM + dom_ids,
        ((group_ids + 1) % N_GROUP) * N_DOM + dom_ids,
    ]
    valid = [
        (dom_ids > 0).astype(jnp.float32),
        (dom_ids < N_DOM - 1).astype(jnp.float32),
        jnp.ones((ndev,), jnp.float32),
        jnp.ones((ndev,), jnp.float32),
    ]
    values = block_values.reshape(ndev, BR_DEV, NB, BS, BS)
    columns = block_cols.reshape(ndev, BR_DEV, NB)
    slot_ids = lax.broadcasted_iota(jnp.int32, (NBLK, NB), 1)
    masks = (slot_ids < live_slots[:, None]).astype(jnp.float32).reshape(ndev, BR_DEV, NB)

    def multiply(vector):
        blocks = vector.reshape(ndev, BR_DEV, BS)
        pieces = [blocks]
        for k in range(4):
            pieces.append(blocks[sources[k][:, None], needed[:, k, :]] * valid[k][:, None, None])
        extended = jnp.concatenate(pieces, axis=1)

        def single(item):
            vals, cols, live, ext = item
            picked = ext[cols] * live[:, :, None]
            return jnp.einsum("bsij,bsj->bi", vals, picked, precision=lax.Precision.HIGHEST)

        return lax.map(single, (values, columns, masks, extended)).reshape(NBLK, BS)

    def advance(vector, theta):
        return multiply(vector) + (diag_shift - theta) * vector

    p_fields = [p_start]
    for step in range(1, S + 1):
        p_fields.append(advance(p_fields[-1], shifts[step - 1]))
    r_fields = [r_start]
    for step in range(1, S):
        r_fields.append(advance(r_fields[-1], shifts[step - 1]))
    basis = jnp.stack(p_fields + r_fields)
    gram = jnp.einsum("kbi,lbi->kl", basis, basis, precision=lax.Precision.HIGHEST) / (NBLK * BS)
    return basis, gram
```

```python
import functools

import jax
import jax.numpy as jnp
from jax import lax
from jax.experimental import pallas as pl
from jax.experimental.pallas import tpu as pltpu
from jax.sharding import PartitionSpec as P

MESH = pl.DeviceIdType.MESH
SUB = 8
PACK = 32


def split(x):
    hi = x.astype(jnp.bfloat16)
    lo = (x - hi.astype(jnp.float32)).astype(jnp.bfloat16)
    return hi, lo


def kernel(n_group, n_dom, shifts_h, cols_h, live_h, needed_h, p_h, r_h, diag_h, a_h, basis, gram,
           shifts, cols, live, needed, a_v, xp0, xp1, xr0, xr1, y0, diag, idx, fields, g_own, g_all, row_own, row_all,
           in_sem, a_sem, send_sem, recv_sem, g_send, g_recv, w_send, w_recv):
    rows, slots, bs, _ = a_v.shape
    depth = shifts.shape[0]
    halo = needed.shape[1]
    count = basis.shape[0]
    width = fields.shape[1]
    loads = a_sem.shape[0]
    per = rows // loads
    groups = rows // SUB
    zero_row = 5 * rows
    n = n_group * n_dom
    g, m = lax.axis_index("group"), lax.axis_index("dom")
    me = g * n_dom + m

    xs = ((xp0, xp1), (xr0, xr1))
    for which in range(2):
        for par in range(2):
            xs[which][par][pl.ds(rows, 2 * rows), :] = jnp.zeros((2 * rows, bs), jnp.float32)
            xs[which][par][pl.ds(zero_row, SUB), :] = jnp.zeros((SUB, bs), jnp.float32)

    barrier = pltpu.get_barrier_semaphore()

    def greet(d, carry):
        to = lax.rem(me + d, n)
        pl.semaphore_signal(barrier, inc=1, device_id=(to // n_dom, lax.rem(to, n_dom)), device_id_type=MESH)
        return carry

    lax.fori_loop(1, n, greet, 0)

    own = pl.ds(0, rows)
    small = (
        (cols_h, cols), (live_h, live), (needed_h, needed), (shifts_h, shifts),
        (p_h, xp0.at[own]), (r_h, xr0.at[own]), (diag_h, diag),
    )

    def small_copy(i):
        return pltpu.make_async_copy(small[i][0], small[i][1], in_sem.at[i])

    def chunk(c):
        part = pl.ds(c * per, per)
        return pltpu.make_async_copy(a_h.at[part], a_v.at[part], a_sem.at[c])

    for i in (4, 5, 0, 1, 2, 3, 6):
        small_copy(i).start()
    for c in range(loads):
        chunk(c).start()

    fields[...] = jnp.zeros_like(fields)

    peers = (
        (g, lax.rem(m + 1, n_dom)),
        (g, lax.rem(m + n_dom - 1, n_dom)),
        (lax.rem(g + 1, n_group), m),
        (lax.rem(g + n_group - 1, n_group), m),
    )

    def copy(which, par, q, k):
        return pltpu.make_async_remote_copy(
            src_ref=xs[which][par].at[pl.ds(q * SUB, SUB)],
            dst_ref=xs[which][par].at[pl.ds((1 + k) * rows + q * SUB, SUB)],
            send_sem=send_sem.at[which, par, q, k],
            recv_sem=recv_sem.at[which, par, q, k],
            device_id=peers[k],
            device_id_type=MESH,
        )

    def guarded(ok, fn):
        if ok is None:
            fn()
        else:
            pl.when(ok)(fn)

    sends = (m < n_dom - 1, m > 0, None, None)
    recvs = (m > 0, m < n_dom - 1, None, None)
    order = (2, 3, 0, 1)

    def both(x, y):
        if x is None:
            return y
        return x if y is None else jnp.logical_and(x, y)

    def start(which, par, q, ok=None):
        for k in order:
            guarded(both(ok, sends[k]), lambda k=k: copy(which, par, q, k).start())

    def wait_send(which, par, ok=None):
        for q in range(groups):
            for k in order:
                guarded(both(ok, sends[k]), lambda q=q, k=k: copy(which, par, q, k).wait_send())

    def wait_recv(which, par):
        for k in (0, 1, 2, 3):
            for q in range(groups):
                guarded(recvs[k], lambda q=q, k=k: copy(which, par, q, k).wait_recv())

    small_copy(4).wait()
    small_copy(5).wait()
    pl.semaphore_wait(barrier, n - 1)
    for which in range(2):
        for q in range(groups):
            start(which, 0, q)

    for i in (0, 1, 2, 3, 6):
        small_copy(i).wait()

    def place(b, carry):
        for s in range(1, slots):
            c = cols[s, b]
            e = jnp.maximum(c - rows, 0)
            k = e // halo
            far = (1 + k) * rows + needed[k, lax.rem(e, halo)]
            at = jnp.where(c < rows, c, far)
            idx[b * slots + s] = jnp.where(s < live[b], at, zero_row)
        return carry

    lax.fori_loop(0, rows, place, 0)

    for which in range(2):
        x = xs[which][0][own, :]
        basis[which * (depth + 1)] = x
        fields[:, which * (depth + 1), :] = x

    def reduced(accs):
        parts = [jnp.transpose(a).reshape(bs // SUB, SUB, bs).sum(axis=0) for a in accs]
        return jnp.stack(parts).sum(axis=1)

    def before(which, par, theta):
        for q in range(groups):
            at = pl.ds(q * SUB, SUB)
            x = xs[which][par][at, :]
            accs = []
            for i in range(SUB):
                b = q * SUB + i
                accs.append(a_v[b, 0] * xs[which][par][pl.ds(b, 1), :])
            y0[which, at, :] = reduced(accs) + (diag[at, :] - theta) * x

    def main(which, par, column, more):
        for q in range(groups):
            at = pl.ds(q * SUB, SUB)
            accs = []
            for i in range(SUB):
                b = q * SUB + i
                acc = None
                for s in range(1, slots):
                    term = a_v[b, s] * xs[which][par][pl.ds(idx[b * slots + s], 1), :]
                    acc = term if acc is None else acc + term
                accs.append(acc)
            y = reduced(accs) + y0[which, at, :]
            if more:
                xs[which][1 - par][at, :] = y
                start(which, 1 - par, q)
            basis[column, at, :] = y
            if more or which == 1:
                fields[at, column, :] = y

    for c in range(loads):
        chunk(c).wait()
    for which in range(2):
        before(which, 0, shifts[0])

    def turn(which, k, par, more, later):
        wait_recv(which, par)
        wait_send(which, 1 - par, later)
        main(which, par, which * (depth + 1) + k, more)
        if more:
            before(which, 1 - par, shifts[k])

    def two(t, carry):
        for par in range(2):
            for which in range(2):
                turn(which, 2 * t + 1 + par, par, True, t > 0 if par == 0 else None)
        return carry

    trips = (depth - 2) // 2
    lax.fori_loop(0, trips, two, 0)
    for k in range(2 * trips + 1, depth):
        for which in range(2):
            turn(which, k, (k - 1) % 2, which == 0 or k < depth - 1, None)

    acc = None
    for b in range(rows):
        hi, lo = split(fields[b])
        pair = jnp.concatenate([hi, lo], axis=0)
        term = lax.dot_general(pair, pair, (((1,), (1,)), ((), ())), preferred_element_type=jnp.float32)
        acc = term if acc is None else acc + term
    top = acc[:width] + acc[width:]
    part = top[:, :width] + top[:, width:]
    wide = jnp.concatenate([part, jnp.zeros((width, bs - width), jnp.float32)], axis=1)
    packed = wide[:SUB]
    for t in range(1, -(-count // SUB)):
        packed = packed + pltpu.roll(wide[t * SUB:(t + 1) * SUB], t * PACK, 1)
    g_own[...] = packed

    def share(d, src, dst, ssem, rsem):
        to = lax.rem(me + d, n)
        return pltpu.make_async_remote_copy(
            src_ref=src, dst_ref=dst.at[me], send_sem=ssem.at[d], recv_sem=rsem.at[me],
            device_id=(to // n_dom, lax.rem(to, n_dom)), device_id_type=MESH,
        )

    def arrival(d, src, dst, ssem, rsem):
        source = lax.rem(me + d, n)
        return pltpu.make_async_remote_copy(
            src_ref=src, dst_ref=dst.at[source], send_sem=ssem.at[0], recv_sem=rsem.at[source],
            device_id=(source // n_dom, lax.rem(source, n_dom)), device_id_type=MESH,
        )

    def each(fn):
        def body(d, carry):
            fn(d)
            return carry
        lax.fori_loop(1, n, body, 0)

    first = (g_own, g_all, g_send, g_recv)
    second = (row_own, row_all, w_send, w_recv)
    each(lambda d: share(d, *first).start())
    g_all[me] = g_own[...]

    wait_recv(0, (depth - 1) % 2)
    main(0, (depth - 1) % 2, depth, False)
    last = basis[depth].reshape(groups, SUB, bs)
    sums = []
    for j in range(width):
        if j < count:
            sums.append((last * basis[j].reshape(groups, SUB, bs)).sum(axis=0))
        else:
            sums.append(jnp.zeros((SUB, bs), jnp.float32))
    flat = jnp.stack(sums).sum(axis=1)
    full = jnp.concatenate([flat, jnp.zeros((bs - width, bs), jnp.float32)], axis=0)
    line = jnp.transpose(full).sum(axis=0, keepdims=True)
    row_own[...] = line
    each(lambda d: share(d, *second).start())
    row_all[me] = line

    each(lambda d: arrival(d, *first).wait_recv())
    total = lax.fori_loop(1, n, lambda i, t: t + g_all[i], g_all[0])
    pieces = [total] + [pltpu.roll(total, bs - t * PACK, 1) for t in range(1, -(-count // SUB))]
    table = jnp.concatenate(pieces, axis=0)
    r_id = lax.broadcasted_iota(jnp.int32, table.shape, 0)
    c_id = lax.broadcasted_iota(jnp.int32, table.shape, 1)
    each(lambda d: arrival(d, *second).wait_recv())
    sweep = row_all[...].reshape(n, bs).sum(axis=0, keepdims=True)
    spread = jnp.broadcast_to(sweep, table.shape)
    side = jnp.where(r_id == c_id, spread, 0.0).sum(axis=1, keepdims=True)
    table = jnp.where(r_id == depth, spread, jnp.where(c_id == depth, side, table))
    gram[...] = table[:count, :count] * (1.0 / (n * rows * bs))

    wait_send(0, 0)
    wait_send(0, 1)
    wait_send(1, (depth - 2) % 2)
    each(lambda d: share(d, *first).wait_send())
    each(lambda d: share(d, *second).wait_send())


def per_device(n_group, n_dom, p_start, r_start, diag_shift, shifts, block_values, block_cols, live_slots, needed):
    rows, bs = p_start.shape
    slots = block_values.shape[1]
    depth = shifts.shape[0]
    halo = needed.shape[2]
    columns = 2 * depth + 1
    width = -(-columns // SUB) * SUB
    n = n_group * n_dom
    loads = rows // 4
    groups = rows // SUB
    hbm = pl.BlockSpec(memory_space=pl.ANY)
    vmem = pl.BlockSpec(memory_space=pltpu.VMEM)
    ext = pltpu.VMEM((5 * rows + SUB, bs), jnp.float32)
    return pl.pallas_call(
        functools.partial(kernel, n_group, n_dom),
        out_shape=(
            jax.ShapeDtypeStruct((columns, rows, bs), jnp.float32),
            jax.ShapeDtypeStruct((columns, columns), jnp.float32),
        ),
        in_specs=[hbm] * 8,
        out_specs=(vmem, vmem),
        scratch_shapes=[
            pltpu.SMEM((depth,), jnp.float32),
            pltpu.SMEM((slots, rows), jnp.int32),
            pltpu.SMEM((rows,), jnp.int32),
            pltpu.SMEM((4, halo), jnp.int32),
            pltpu.VMEM(block_values.shape, jnp.float32),
            ext, ext, ext, ext,
            pltpu.VMEM((2, rows, bs), jnp.float32),
            pltpu.VMEM((rows, bs), jnp.float32),
            pltpu.SMEM((rows * slots,), jnp.int32),
            pltpu.VMEM((rows, width, bs), jnp.float32),
            pltpu.VMEM((SUB, bs), jnp.float32),
            pltpu.VMEM((n, SUB, bs), jnp.float32),
            pltpu.VMEM((1, bs), jnp.float32),
            pltpu.VMEM((n, 1, bs), jnp.float32),
            pltpu.SemaphoreType.DMA((7,)),
            pltpu.SemaphoreType.DMA((loads,)),
            pltpu.SemaphoreType.DMA((2, 2, groups, 4)),
            pltpu.SemaphoreType.DMA((2, 2, groups, 4)),
            pltpu.SemaphoreType.DMA((n,)),
            pltpu.SemaphoreType.DMA((n,)),
            pltpu.SemaphoreType.DMA((n,)),
            pltpu.SemaphoreType.DMA((n,)),
        ],
        compiler_params=pltpu.CompilerParams(
            collective_id=0, has_side_effects=True, vmem_limit_bytes=60 * 1024 * 1024
        ),
    )(shifts, block_cols.T, live_slots, needed[0], p_start, r_start, diag_shift, block_values)


def solution(mesh):
    return jax.shard_map(
        functools.partial(per_device, mesh.shape["group"], mesh.shape["dom"]),
        mesh=mesh,
        in_specs=(
            P(("group", "dom"), None),
            P(("group", "dom"), None),
            P(("group", "dom"), None),
            P(),
            P(("group", "dom"), None, None, None),
            P(("group", "dom"), None),
            P(("group", "dom")),
            P(("group", "dom"), None, None),
        ),
        out_specs=(P(None, ("group", "dom"), None), P()),
        check_vma=False,
    )
```

```python
import functools

import jax
import jax.numpy as jnp
from jax import lax
from jax.experimental import pallas as pl
from jax.experimental.pallas import tpu as pltpu
from jax.sharding import PartitionSpec as P

MESH = pl.DeviceIdType.MESH
SUB = 8
PACK = 32


def split(x):
    hi = x.astype(jnp.bfloat16)
    lo = (x - hi.astype(jnp.float32)).astype(jnp.bfloat16)
    return hi, lo


def kernel(n_group, n_dom, shifts_h, cols_h, live_h, needed_h, p_h, r_h, diag_h, a_h, basis, gram,
           shifts, cols, live, needed, a_v, xp0, xp1, xr0, xr1, y0, diag, idx, fields, g_own, g_all, row_own, row_all,
           in_sem, a_sem, send_sem, recv_sem, g_send, g_recv):
    rows, slots, bs, _ = a_v.shape
    depth = shifts.shape[0]
    halo = needed.shape[1]
    count = basis.shape[0]
    width = fields.shape[1]
    groups = rows // SUB
    zero_row = 5 * rows
    n = n_group * n_dom
    g, m = lax.axis_index("group"), lax.axis_index("dom")
    me = g * n_dom + m

    xs = ((xp0, xp1), (xr0, xr1))
    for which in range(2):
        for par in range(2):
            xs[which][par][pl.ds(rows, 2 * rows), :] = jnp.zeros((2 * rows, bs), jnp.float32)
            xs[which][par][pl.ds(zero_row, SUB), :] = jnp.zeros((SUB, bs), jnp.float32)

    peers = (
        (g, lax.rem(m + 1, n_dom)),
        (g, lax.rem(m + n_dom - 1, n_dom)),
        (lax.rem(g + 1, n_group), m),
        (lax.rem(g + n_group - 1, n_group), m),
    )
    sends = (m < n_dom - 1, m > 0, None, None)
    order = (2, 3, 0, 1)
    inner = jnp.logical_and(m > 0, m < n_dom - 1)
    others = [(a, b) for a in range(n_group) for b in range(n_dom) if a + b > 0]

    def at_offset(a, b):
        return lax.rem(g + a, n_group), lax.rem(m + b, n_dom)

    def guarded(ok, fn):
        if ok is None:
            fn()
        else:
            pl.when(ok)(fn)

    barrier = pltpu.get_barrier_semaphore()
    near = n_dom - 1 + n_group // 2 <= depth + 1
    if near:
        for k in order:
            guarded(sends[k], lambda k=k: pl.semaphore_signal(
                barrier, inc=1, device_id=peers[k], device_id_type=MESH))
    else:
        for a, b in others:
            pl.semaphore_signal(barrier, inc=1, device_id=at_offset(a, b), device_id_type=MESH)

    own = pl.ds(0, rows)
    small = (
        (p_h, xp0.at[own]), (r_h, xr0.at[own]), (cols_h, cols), (live_h, live), (needed_h, needed),
        (shifts_h, shifts), (diag_h, diag),
    )

    def small_copy(i):
        return pltpu.make_async_copy(small[i][0], small[i][1], in_sem.at[i])

    def chunk(c):
        part = pl.ds(0, 1) if c == 0 else pl.ds(1, slots - 1)
        return pltpu.make_async_copy(a_h.at[:, part], a_v.at[:, part], a_sem.at[c])

    for i in range(len(small)):
        small_copy(i).start()
    for c in range(2):
        chunk(c).start()

    def copy(which, par, q, k):
        return pltpu.make_async_remote_copy(
            src_ref=xs[which][par].at[pl.ds(q * SUB, SUB)],
            dst_ref=xs[which][par].at[pl.ds((1 + k) * rows + q * SUB, SUB)],
            send_sem=send_sem.at[which, par],
            recv_sem=recv_sem.at[which, par],
            device_id=peers[k],
            device_id_type=MESH,
        )

    def start(which, par, q):
        for k in order:
            guarded(sends[k], lambda k=k: copy(which, par, q, k).start())

    def halos(which, par, count):
        part = xs[which][par].at[pl.ds(rows, count * rows)]
        return pltpu.make_async_remote_copy(
            src_ref=part, dst_ref=part, send_sem=send_sem.at[which, par], recv_sem=recv_sem.at[which, par],
            device_id=peers[2], device_id_type=MESH,
        )

    def wait_send(which, par, ok=None):
        for count, side in ((4, inner), (3, jnp.logical_not(inner))):
            pl.when(side if ok is None else jnp.logical_and(ok, side))(
                lambda count=count: halos(which, par, count).wait_send())

    def wait_recv(which, par):
        for count, side in ((4, inner), (3, jnp.logical_not(inner))):
            pl.when(side)(lambda count=count: halos(which, par, count).wait_recv())

    fields[...] = jnp.zeros_like(fields)
    small_copy(0).wait()
    small_copy(1).wait()
    pl.semaphore_wait(barrier, jnp.where(inner, 4, 3) if near else n - 1)
    for which in range(2):
        for q in range(groups):
            start(which, 0, q)

    for i in range(2, len(small)):
        small_copy(i).wait()

    def place(b, carry):
        for s in range(1, slots):
            c = cols[s, b]
            e = jnp.maximum(c - rows, 0)
            k = e // halo
            far = (1 + k) * rows + needed[k, lax.rem(e, halo)]
            at = jnp.where(c < rows, c, far)
            idx[b * slots + s] = jnp.where(s < live[b], at, zero_row)
        return carry

    lax.fori_loop(0, rows, place, 0)

    for which in range(2):
        x = xs[which][0][own, :]
        basis[which * (depth + 1)] = x
        fields[:, which * (depth + 1), :] = x

    def folded(acc):
        return jnp.transpose(acc).reshape(bs // SUB, SUB, bs).sum(axis=0)

    def before(which, par, theta):
        x = xs[which][par]
        for q in range(groups):
            at = pl.ds(q * SUB, SUB)
            parts = [folded(a_v[q * SUB + i, 0] * x[pl.ds(q * SUB + i, 1), :]) for i in range(SUB)]
            y0[which, at, :] = jnp.stack(parts).sum(axis=1) + (diag[at, :] - theta) * x[at, :]

    def main(which, par, column, more):
        x = xs[which][par]

        def row(b):
            acc = None
            for s in range(1, slots):
                term = a_v[b, s] * x[pl.ds(idx[b * slots + s], 1), :]
                acc = term if acc is None else acc + term
            return folded(acc)

        def finish(q, parts):
            at = pl.ds(q * SUB, SUB)
            y = jnp.stack(parts).sum(axis=1) + y0[which, at, :]
            if more:
                xs[which][1 - par][at, :] = y
                start(which, 1 - par, q)
            basis[column, at, :] = y
            if more or which == 1:
                fields[at, column, :] = y

        held = None
        for q in range(groups):
            parts = []
            for i in range(SUB):
                parts.append(row(q * SUB + i))
                if held is not None and i == SUB // 2 - 1:
                    finish(q - 1, held)
            held = parts
        finish(groups - 1, held)

    chunk(0).wait()
    for which in range(2):
        before(which, 0, shifts[0])
    chunk(1).wait()

    def turn(which, k, par, more, later):
        wait_recv(which, par)
        wait_send(which, 1 - par, later)
        main(which, par, which * (depth + 1) + k, more)
        if more:
            before(which, 1 - par, shifts[k])

    def two(t, carry):
        for par in range(2):
            for which in range(2):
                turn(which, 2 * t + 1 + par, par, True, t > 0 if par == 0 else None)
        return carry

    trips = (depth - 2) // 2
    lax.fori_loop(0, trips, two, 0)
    for k in range(2 * trips + 1, depth):
        for which in range(2):
            turn(which, k, (k - 1) % 2, which == 0 or k < depth - 1, None)

    acc = None
    for b in range(rows):
        hi, lo = split(fields[b])
        pair = jnp.concatenate([hi, lo], axis=0)
        term = lax.dot_general(pair, pair, (((1,), (1,)), ((), ())), preferred_element_type=jnp.float32)
        acc = term if acc is None else acc + term
    top = acc[:width] + acc[width:]
    part = top[:, :width] + top[:, width:]
    wide = jnp.concatenate([part, jnp.zeros((width, bs - width), jnp.float32)], axis=1)
    packed = wide[:SUB]
    for t in range(1, -(-count // SUB)):
        packed = packed + pltpu.roll(wide[t * SUB:(t + 1) * SUB], t * PACK, 1)
    g_own[...] = packed

    def share(a, b, src, dst, i):
        return pltpu.make_async_remote_copy(
            src_ref=src, dst_ref=dst.at[me], send_sem=g_send.at[i], recv_sem=g_recv.at[i],
            device_id=at_offset(a, b), device_id_type=MESH,
        )

    def shared(dst, i):
        part = dst.at[pl.ds(0, n - 1)]
        return pltpu.make_async_remote_copy(
            src_ref=part, dst_ref=part, send_sem=g_send.at[i], recv_sem=g_recv.at[i],
            device_id=peers[2], device_id_type=MESH,
        )

    wait_recv(0, (depth - 1) % 2)
    for a, b in others:
        share(a, b, g_own, g_all, 0).start()
    g_all[me] = g_own[...]
    main(0, (depth - 1) % 2, depth, False)
    last = basis[depth].reshape(groups, SUB, bs)
    sums = []
    for j in range(width):
        if j < count:
            sums.append((last * basis[j].reshape(groups, SUB, bs)).sum(axis=0))
        else:
            sums.append(jnp.zeros((SUB, bs), jnp.float32))
    flat = jnp.stack(sums).sum(axis=1)
    full = jnp.concatenate([flat, jnp.zeros((bs - width, bs), jnp.float32)], axis=0)
    line = jnp.transpose(full).sum(axis=0, keepdims=True)
    row_own[...] = line
    for a, b in others:
        share(a, b, row_own, row_all, 1).start()
    row_all[me] = line

    shared(g_all, 0).wait_recv()
    total = g_all[...].sum(axis=0)
    pieces = [total] + [pltpu.roll(total, bs - t * PACK, 1) for t in range(1, -(-count // SUB))]
    table = jnp.concatenate(pieces, axis=0)
    r_id = lax.broadcasted_iota(jnp.int32, table.shape, 0)
    c_id = lax.broadcasted_iota(jnp.int32, table.shape, 1)
    shared(row_all, 1).wait_recv()
    sweep = row_all[...].reshape(n, bs).sum(axis=0, keepdims=True)
    spread = jnp.broadcast_to(sweep, table.shape)
    side = jnp.where(r_id == c_id, spread, 0.0).sum(axis=1, keepdims=True)
    table = jnp.where(r_id == depth, spread, jnp.where(c_id == depth, side, table))
    gram[...] = table[:count, :count] * (1.0 / (n * rows * bs))

    wait_send(0, 0)
    wait_send(0, 1)
    wait_send(1, (depth - 2) % 2)
    shared(g_all, 0).wait_send()
    shared(row_all, 1).wait_send()


def export(b_ref, g_ref, b_out, g_out, sem):
    copies = [pltpu.make_async_copy(b_ref, b_out, sem.at[0]), pltpu.make_async_copy(g_ref, g_out, sem.at[1])]
    for c in copies:
        c.start()
    for c in copies:
        c.wait()


def per_device(n_group, n_dom, p_start, r_start, diag_shift, shifts, block_values, block_cols, live_slots, needed):
    rows, bs = p_start.shape
    slots = block_values.shape[1]
    depth = shifts.shape[0]
    halo = needed.shape[2]
    columns = 2 * depth + 1
    width = -(-columns // SUB) * SUB
    n = n_group * n_dom
    hbm = pl.BlockSpec(memory_space=pltpu.HBM)
    vmem = pl.BlockSpec(memory_space=pltpu.VMEM)
    ext = pltpu.VMEM((5 * rows + SUB, bs), jnp.float32)
    basis, gram = pl.pallas_call(
        functools.partial(kernel, n_group, n_dom),
        out_shape=(
            jax.ShapeDtypeStruct((columns, rows, bs), jnp.float32),
            jax.ShapeDtypeStruct((columns, columns), jnp.float32),
        ),
        in_specs=[hbm] * 8,
        out_specs=(vmem, vmem),
        scratch_shapes=[
            pltpu.SMEM((depth,), jnp.float32),
            pltpu.SMEM((slots, rows), jnp.int32),
            pltpu.SMEM((rows,), jnp.int32),
            pltpu.SMEM((4, halo), jnp.int32),
            pltpu.VMEM(block_values.shape, jnp.float32),
            ext, ext, ext, ext,
            pltpu.VMEM((2, rows, bs), jnp.float32),
            pltpu.VMEM((rows, bs), jnp.float32),
            pltpu.SMEM((rows * slots,), jnp.int32),
            pltpu.VMEM((rows, width, bs), jnp.float32),
            pltpu.VMEM((SUB, bs), jnp.float32),
            pltpu.VMEM((n, SUB, bs), jnp.float32),
            pltpu.VMEM((1, bs), jnp.float32),
            pltpu.VMEM((n, 1, bs), jnp.float32),
            pltpu.SemaphoreType.DMA((7,)),
            pltpu.SemaphoreType.DMA((2,)),
            pltpu.SemaphoreType.DMA((2, 2)),
            pltpu.SemaphoreType.DMA((2, 2)),
            pltpu.SemaphoreType.DMA((2,)),
            pltpu.SemaphoreType.DMA((2,)),
        ],
        compiler_params=pltpu.CompilerParams(
            collective_id=0, has_side_effects=True, vmem_limit_bytes=24 * 1024 * 1024
        ),
    )(*[pltpu.with_memory_space_constraint(v, pltpu.HBM) for v in (
        shifts, block_cols.T, live_slots, needed[0], p_start, r_start, diag_shift, block_values)])
    return pl.pallas_call(
        export,
        out_shape=(
            jax.ShapeDtypeStruct(basis.shape, jnp.float32),
            jax.ShapeDtypeStruct(gram.shape, jnp.float32),
        ),
        in_specs=[vmem, vmem],
        out_specs=(hbm, hbm),
        scratch_shapes=[pltpu.SemaphoreType.DMA((2,))],
        compiler_params=pltpu.CompilerParams(vmem_limit_bytes=4 * 1024 * 1024),
    )(basis, gram)


def solution(mesh):
    return jax.shard_map(
        functools.partial(per_device, mesh.shape["group"], mesh.shape["dom"]),
        mesh=mesh,
        in_specs=(
            P(("group", "dom"), None),
            P(("group", "dom"), None),
            P(("group", "dom"), None),
            P(),
            P(("group", "dom"), None, None, None),
            P(("group", "dom"), None),
            P(("group", "dom")),
            P(("group", "dom"), None, None),
        ),
        out_specs=(P(None, ("group", "dom"), None), P()),
        check_vma=False,
    )
```

```python
import functools

import jax
import jax.numpy as jnp
from jax import lax
from jax.experimental import pallas as pl
from jax.experimental.pallas import tpu as pltpu
from jax.sharding import PartitionSpec as P

MESH = pl.DeviceIdType.MESH
SUB = 8
PACK = 32
MXU_ROWS = 8


def split(x):
    hi = x.astype(jnp.bfloat16)
    lo = (x - hi.astype(jnp.float32)).astype(jnp.bfloat16)
    return hi, lo


def kernel(n_group, n_dom, shifts_h, cols_h, live_h, needed_h, p_h, r_h, diag_h, a_h, basis, gram,
           shifts, cols, live, needed, a_v, w_v, xp0, xp1, xr0, xr1, y0, diag, idx, spot, fields, g_own, g_all, row_own, row_all,
           in_sem, a_sem, send_sem, recv_sem, g_send, g_recv):
    rows, slots, bs, _ = a_v.shape
    depth = shifts.shape[0]
    halo = needed.shape[1]
    count = basis.shape[0]
    width = fields.shape[1]
    groups = rows // SUB
    zero_row = 5 * rows
    n = n_group * n_dom
    g, m = lax.axis_index("group"), lax.axis_index("dom")
    me = g * n_dom + m

    xs = ((xp0, xp1), (xr0, xr1))
    for which in range(2):
        for par in range(2):
            xs[which][par][pl.ds(rows, 2 * rows), :] = jnp.zeros((2 * rows, bs), jnp.float32)
            xs[which][par][pl.ds(zero_row, SUB), :] = jnp.zeros((SUB, bs), jnp.float32)

    peers = (
        (g, lax.rem(m + 1, n_dom)),
        (g, lax.rem(m + n_dom - 1, n_dom)),
        (lax.rem(g + 1, n_group), m),
        (lax.rem(g + n_group - 1, n_group), m),
    )
    sends = (m < n_dom - 1, m > 0, None, None)
    order = (2, 3, 0, 1)
    inner = jnp.logical_and(m > 0, m < n_dom - 1)
    others = [(a, b) for b in range(n_dom) for a in range(n_group) if a + b > 0]
    others.sort(key=lambda o: -min(o[1], n_dom - o[1]))

    def at_offset(a, b):
        return lax.rem(g + a, n_group), lax.rem(m + b, n_dom)

    def guarded(ok, fn):
        if ok is None:
            fn()
        else:
            pl.when(ok)(fn)

    barrier = pltpu.get_barrier_semaphore()
    near = n_dom <= depth
    if near:
        for a in range(1, n_group):
            pl.semaphore_signal(barrier, inc=1, device_id=at_offset(a, 0), device_id_type=MESH)
        for k in (0, 1):
            guarded(sends[k], lambda k=k: pl.semaphore_signal(
                barrier, inc=1, device_id=peers[k], device_id_type=MESH))
    else:
        for a, b in others:
            pl.semaphore_signal(barrier, inc=1, device_id=at_offset(a, b), device_id_type=MESH)

    own = pl.ds(0, rows)
    small = (
        (p_h, xp0.at[own]), (r_h, xr0.at[own]), (cols_h, cols), (live_h, live), (needed_h, needed),
        (shifts_h, shifts), (diag_h, diag),
    )

    def small_copy(i):
        return pltpu.make_async_copy(small[i][0], small[i][1], in_sem.at[i])

    def chunk(c):
        part = (
            (slice(None), pl.ds(0, 1)),
            (pl.ds(0, MXU_ROWS), pl.ds(1, slots - 1)),
            (pl.ds(MXU_ROWS, rows - MXU_ROWS), pl.ds(1, slots - 1)),
        )[c]
        return pltpu.make_async_copy(a_h.at[part], a_v.at[part], a_sem.at[c])

    for i in range(len(small)):
        small_copy(i).start()
    for c in range(3):
        chunk(c).start()

    def copy(which, par, q, k):
        return pltpu.make_async_remote_copy(
            src_ref=xs[which][par].at[pl.ds(q * SUB, SUB)],
            dst_ref=xs[which][par].at[pl.ds((1 + k) * rows + q * SUB, SUB)],
            send_sem=send_sem.at[which, par],
            recv_sem=recv_sem.at[which, par],
            device_id=peers[k],
            device_id_type=MESH,
        )

    def start(which, par, q):
        for k in order:
            guarded(sends[k], lambda k=k: copy(which, par, q, k).start())

    def halos(which, par, count):
        part = xs[which][par].at[pl.ds(rows, count * rows)]
        return pltpu.make_async_remote_copy(
            src_ref=part, dst_ref=part, send_sem=send_sem.at[which, par], recv_sem=recv_sem.at[which, par],
            device_id=peers[2], device_id_type=MESH,
        )

    def wait_send(which, par, ok=None):
        for count, side in ((4, inner), (3, jnp.logical_not(inner))):
            pl.when(side if ok is None else jnp.logical_and(ok, side))(
                lambda count=count: halos(which, par, count).wait_send())

    def wait_recv(which, par):
        for count, side in ((4, inner), (3, jnp.logical_not(inner))):
            pl.when(side)(lambda count=count: halos(which, par, count).wait_recv())

    fields[...] = jnp.zeros_like(fields)
    small_copy(0).wait()
    small_copy(1).wait()
    pl.semaphore_wait(barrier, n_group + inner.astype(jnp.int32) if near else n - 1)
    for which in range(2):
        for q in range(groups):
            start(which, 0, q)

    for i in range(2, len(small)):
        small_copy(i).wait()
    for c in range(rows):
        spot[c] = c
    for k in range(4):
        for h in range(halo):
            spot[rows + k * halo + h] = (1 + k) * rows + needed[k, h]
    for b in range(rows):
        used = live[b]
        for s in range(1, slots):
            idx[b * slots + s] = jnp.where(s < used, spot[cols[s, b]], zero_row)

    for which in range(2):
        x = xs[which][0][own, :]
        basis[which * (depth + 1)] = x
        fields[:, which * (depth + 1), :] = x

    def folded(acc):
        return jnp.transpose(acc).reshape(bs // SUB, SUB, bs).sum(axis=0)

    def before(which, par, theta):
        x = xs[which][par]
        for q in range(groups):
            at = pl.ds(q * SUB, SUB)
            parts = [folded(a_v[q * SUB + i, 0] * x[pl.ds(q * SUB + i, 1), :]) for i in range(SUB)]
            y0[which, at, :] = jnp.stack(parts).sum(axis=1) + (diag[at, :] - theta) * x[at, :]

    def main(which, par, column, more, keep):
        x = xs[which][par]

        def row(b):
            acc = None
            for s in range(1, slots):
                term = a_v[b, s] * x[pl.ds(idx[b * slots + s], 1), :]
                acc = term if acc is None else acc + term
            return folded(acc)

        def finish(q, parts):
            at = pl.ds(q * SUB, SUB)
            y = jnp.stack(parts).sum(axis=1) + y0[which, at, :]
            if more:
                xs[which][1 - par][at, :] = y
                start(which, 1 - par, q)
            basis[column, at, :] = y
            if keep:
                fields[at, column, :] = y

        sub = lax.broadcasted_iota(jnp.int32, (SUB, bs), 0)

        def pair(p):
            acc = None
            for s in range(1, slots):
                v = jnp.where(
                    sub < 2,
                    x[pl.ds(idx[2 * p * slots + s], 1), :],
                    x[pl.ds(idx[(2 * p + 1) * slots + s], 1), :],
                )
                hi = v.astype(jnp.bfloat16).astype(jnp.float32)
                lhs = jnp.where(sub % 2 == 0, hi, v - hi).astype(jnp.bfloat16)
                term = jnp.dot(
                    jnp.concatenate([lhs, lhs], axis=1), w_v[p, s - 1], preferred_element_type=jnp.float32
                )
                acc = term if acc is None else acc + term
            return [
                jnp.where(sub < 2, acc[:, :bs], 0.0),
                jnp.where(sub // 2 == 1, acc[:, bs:], 0.0),
            ]

        parts = {}
        held = []
        todo = list(range(MXU_ROWS, rows))
        done = 0
        for p in range(MXU_ROWS // 2):
            parts[2 * p], parts[2 * p + 1] = pair(p)
            stop = (p + 1) * len(todo) // (MXU_ROWS // 2) if p + 1 < MXU_ROWS // 2 else len(todo)
            for b in todo[done:stop]:
                parts[b] = row(b)
                if b % SUB == SUB // 2 - 1 and held:
                    finish(held[0], [parts[held[0] * SUB + i] for i in range(SUB)])
                    held = held[1:]
                if b % SUB == SUB - 1:
                    held.append(b // SUB)
            done = stop
        for q in [h for h in held] + [q for q in range(groups) if (q + 1) * SUB <= MXU_ROWS]:
            finish(q, [parts[q * SUB + i] for i in range(SUB)])

    chunk(0).wait()
    for which in range(2):
        before(which, 0, shifts[0])
    chunk(1).wait()

    def weights(p, carry):
        for s in range(1, slots):
            for e in range(2):
                t = jnp.transpose(a_v[2 * p + e, s])
                hi, lo = split(t)
                w_v[p, s - 1, pl.ds(0, bs), pl.ds(e * bs, bs)] = hi
                w_v[p, s - 1, pl.ds(bs, bs), pl.ds(e * bs, bs)] = lo
        return carry

    lax.fori_loop(0, MXU_ROWS // 2, weights, 0)
    chunk(2).wait()

    def turn(which, k, par, more, later, keep=True):
        wait_recv(which, par)
        wait_send(which, 1 - par, later)
        main(which, par, which * (depth + 1) + k, more, keep)
        if more:
            before(which, 1 - par, shifts[k])

    def two(t, carry):
        for par in range(2):
            for which in range(2):
                turn(which, 2 * t + 1 + par, par, True, t > 0 if par == 0 else None)
        return carry

    trips = (depth - 2) // 2
    lax.fori_loop(0, trips, two, 0)
    for k in range(2 * trips + 1, depth - 1):
        for which in range(2):
            turn(which, k, (k - 1) % 2, which == 0 or k < depth - 1, None)

    def share(a, b, src, dst, i):
        return pltpu.make_async_remote_copy(
            src_ref=src, dst_ref=dst.at[me], send_sem=g_send.at[i], recv_sem=g_recv.at[i],
            device_id=at_offset(a, b), device_id_type=MESH,
        )

    def shared(dst, i):
        part = dst.at[pl.ds(0, n - 1)]
        return pltpu.make_async_remote_copy(
            src_ref=part, dst_ref=part, send_sem=g_send.at[i], recv_sem=g_recv.at[i],
            device_id=peers[2], device_id_type=MESH,
        )

    turn(0, depth - 1, depth % 2, True, None, False)
    acc = None
    for b in range(rows):
        hi, lo = split(fields[b])
        pair = jnp.concatenate([hi, lo], axis=0)
        term = lax.dot_general(pair, pair, (((1,), (1,)), ((), ())), preferred_element_type=jnp.float32)
        acc = term if acc is None else acc + term
    top = acc[:width] + acc[width:]
    part = top[:, :width] + top[:, width:]
    wide = jnp.concatenate([part, jnp.zeros((width, bs - width), jnp.float32)], axis=1)
    packed = wide[:SUB]
    for t in range(1, -(-count // SUB)):
        packed = packed + pltpu.roll(wide[t * SUB:(t + 1) * SUB], t * PACK, 1)
    g_own[...] = packed

    for a, b in others:
        share(a, b, g_own, g_all, 0).start()
    g_all[me] = g_own[...]
    turn(1, depth - 1, depth % 2, False, None, False)

    late = (depth - 1, 2 * depth, depth)

    def products(c, known):
        x = basis[c].reshape(groups, SUB, bs)
        sums = []
        for j in range(PACK):
            if j in known:
                sums.append((x * basis[j].reshape(groups, SUB, bs)).sum(axis=0))
            else:
                sums.append(jnp.zeros((SUB, bs), jnp.float32))
        return jnp.stack(sums).sum(axis=1)

    seen = [j for j in range(count) if j != depth]
    halves = [products(late[0], seen), products(late[1], seen)]
    early = jnp.transpose(jnp.concatenate(halves + [jnp.zeros((bs - 2 * PACK, bs), jnp.float32)], axis=0))
    early = early.sum(axis=0, keepdims=True)

    wait_recv(0, (depth - 1) % 2)
    main(0, (depth - 1) % 2, depth, False, False)
    pad = jnp.zeros((2 * PACK, bs), jnp.float32)
    end = jnp.concatenate([pad, products(depth, list(range(count))), pad[:bs - 3 * PACK]], axis=0)
    line = jnp.transpose(end).sum(axis=0, keepdims=True) + early
    row_own[...] = line
    for a, b in others:
        share(a, b, row_own, row_all, 1).start()
    row_all[me] = line

    shared(g_all, 0).wait_recv()
    total = g_all[...].sum(axis=0)
    pieces = [total] + [pltpu.roll(total, bs - t * PACK, 1) for t in range(1, -(-count // SUB))]
    table = jnp.concatenate(pieces, axis=0)
    r_id = lax.broadcasted_iota(jnp.int32, table.shape, 0)
    c_id = lax.broadcasted_iota(jnp.int32, table.shape, 1)
    shared(row_all, 1).wait_recv()
    sweep = jnp.broadcast_to(row_all[...].reshape(n, bs).sum(axis=0, keepdims=True), table.shape)
    for i in (1, 0, 2):
        c = late[i]
        across = sweep if i == 0 else pltpu.roll(sweep, bs - i * PACK, 1)
        down = jnp.where(c_id == r_id + i * PACK, sweep, 0.0).sum(axis=1, keepdims=True)
        table = jnp.where(r_id == c, across, jnp.where(c_id == c, down, table))
    gram[...] = table[:count, :count] * (1.0 / (n * rows * bs))

    wait_send(0, 0)
    wait_send(0, 1)
    wait_send(1, (depth - 2) % 2)
    shared(g_all, 0).wait_send()
    shared(row_all, 1).wait_send()


def export(b_ref, g_ref, b_out, g_out, sem):
    copies = [pltpu.make_async_copy(b_ref, b_out, sem.at[0]), pltpu.make_async_copy(g_ref, g_out, sem.at[1])]
    for c in copies:
        c.start()
    for c in copies:
        c.wait()


def per_device(n_group, n_dom, p_start, r_start, diag_shift, shifts, block_values, block_cols, live_slots, needed):
    rows, bs = p_start.shape
    slots = block_values.shape[1]
    depth = shifts.shape[0]
    halo = needed.shape[2]
    columns = 2 * depth + 1
    width = -(-columns // SUB) * SUB
    n = n_group * n_dom
    hbm = pl.BlockSpec(memory_space=pltpu.HBM)
    vmem = pl.BlockSpec(memory_space=pltpu.VMEM)
    ext = pltpu.VMEM((5 * rows + SUB, bs), jnp.float32)
    basis, gram = pl.pallas_call(
        functools.partial(kernel, n_group, n_dom),
        out_shape=(
            jax.ShapeDtypeStruct((columns, rows, bs), jnp.float32),
            jax.ShapeDtypeStruct((columns, columns), jnp.float32),
        ),
        in_specs=[hbm] * 8,
        out_specs=(vmem, vmem),
        scratch_shapes=[
            pltpu.SMEM((depth,), jnp.float32),
            pltpu.SMEM((slots, rows), jnp.int32),
            pltpu.SMEM((rows,), jnp.int32),
            pltpu.SMEM((4, halo), jnp.int32),
            pltpu.VMEM(block_values.shape, jnp.float32),
            pltpu.VMEM((MXU_ROWS // 2, slots - 1, 2 * bs, 2 * bs), jnp.bfloat16),
            ext, ext, ext, ext,
            pltpu.VMEM((2, rows, bs), jnp.float32),
            pltpu.VMEM((rows, bs), jnp.float32),
            pltpu.SMEM((rows * slots,), jnp.int32),
            pltpu.SMEM((rows + 4 * halo,), jnp.int32),
            pltpu.VMEM((rows, width, bs), jnp.float32),
            pltpu.VMEM((SUB, bs), jnp.float32),
            pltpu.VMEM((n, SUB, bs), jnp.float32),
            pltpu.VMEM((1, bs), jnp.float32),
            pltpu.VMEM((n, 1, bs), jnp.float32),
            pltpu.SemaphoreType.DMA((7,)),
            pltpu.SemaphoreType.DMA((3,)),
            pltpu.SemaphoreType.DMA((2, 2)),
            pltpu.SemaphoreType.DMA((2, 2)),
            pltpu.SemaphoreType.DMA((2,)),
            pltpu.SemaphoreType.DMA((2,)),
        ],
        compiler_params=pltpu.CompilerParams(
            collective_id=0, has_side_effects=True, vmem_limit_bytes=24 * 1024 * 1024
        ),
    )(*[pltpu.with_memory_space_constraint(v, pltpu.HBM) for v in (
        shifts, block_cols.T, live_slots, needed[0], p_start, r_start, diag_shift, block_values)])
    return pl.pallas_call(
        export,
        out_shape=(
            jax.ShapeDtypeStruct(basis.shape, jnp.float32),
            jax.ShapeDtypeStruct(gram.shape, jnp.float32),
        ),
        in_specs=[vmem, vmem],
        out_specs=(hbm, hbm),
        scratch_shapes=[pltpu.SemaphoreType.DMA((2,))],
        compiler_params=pltpu.CompilerParams(vmem_limit_bytes=4 * 1024 * 1024),
    )(basis, gram)


def solution(mesh):
    return jax.shard_map(
        functools.partial(per_device, mesh.shape["group"], mesh.shape["dom"]),
        mesh=mesh,
        in_specs=(
            P(("group", "dom"), None),
            P(("group", "dom"), None),
            P(("group", "dom"), None),
            P(),
            P(("group", "dom"), None, None, None),
            P(("group", "dom"), None),
            P(("group", "dom")),
            P(("group", "dom"), None, None),
        ),
        out_specs=(P(None, ("group", "dom"), None), P()),
        check_vma=False,
    )
```

```python
import functools

import jax
import jax.numpy as jnp
from jax import lax
from jax.experimental import pallas as pl
from jax.experimental.pallas import tpu as pltpu
from jax.sharding import PartitionSpec as P

MESH = pl.DeviceIdType.MESH
SUB = 8
PACK = 32
MXU_ROWS = 8


def split(x):
    hi = x.astype(jnp.bfloat16)
    lo = (x - hi.astype(jnp.float32)).astype(jnp.bfloat16)
    return hi, lo


def kernel(n_group, n_dom, shifts_h, cols_h, live_h, needed_h, p_h, r_h, diag_h, a_h, basis, gram,
           shifts, cols, live, needed, a_v, w_v, xp0, xp1, xr0, xr1, y0, diag, idx, spot, want, fresh, outbox, fields, g_own, g_all, row_own, row_all,
           in_sem, a_sem, send_sem, recv_sem, g_send, g_recv, l_send, l_recv):
    rows, slots, bs, _ = a_v.shape
    depth = shifts.shape[0]
    halo = needed.shape[1]
    count = basis.shape[0]
    width = fields.shape[1]
    groups = rows // SUB
    zero_row = 5 * rows
    n = n_group * n_dom
    g, m = lax.axis_index("group"), lax.axis_index("dom")
    me = g * n_dom + m

    xs = ((xp0, xp1), (xr0, xr1))
    for which in range(2):
        for par in range(2):
            xs[which][par][pl.ds(rows, 2 * rows), :] = jnp.zeros((2 * rows, bs), jnp.float32)
            xs[which][par][pl.ds(zero_row, SUB), :] = jnp.zeros((SUB, bs), jnp.float32)

    for k in range(2):
        for h in range(halo):
            want[k, k, h] = 0

    peers = (
        (g, lax.rem(m + 1, n_dom)),
        (g, lax.rem(m + n_dom - 1, n_dom)),
        (lax.rem(g + 1, n_group), m),
        (lax.rem(g + n_group - 1, n_group), m),
    )
    sends = (m < n_dom - 1, m > 0, None, None)
    order = (2, 3, 0, 1)
    inner = jnp.logical_and(m > 0, m < n_dom - 1)
    others = [(a, b) for b in range(n_dom) for a in range(n_group) if a + b > 0]
    others.sort(key=lambda o: (o[1] == 0, o[1], -abs(o[0] - n_group / 2 + 0.5)))

    def at_offset(a, b):
        return lax.rem(g + a, n_group), lax.rem(m + b, n_dom)

    def guarded(ok, fn):
        if ok is None:
            fn()
        else:
            pl.when(ok)(fn)

    barrier = pltpu.get_barrier_semaphore()
    near = n_dom <= depth
    if near:
        for a in range(1, n_group):
            pl.semaphore_signal(barrier, inc=1, device_id=at_offset(a, 0), device_id_type=MESH)
        for k in (0, 1):
            guarded(sends[k], lambda k=k: pl.semaphore_signal(
                barrier, inc=1, device_id=peers[k], device_id_type=MESH))
    else:
        for a, b in others:
            pl.semaphore_signal(barrier, inc=1, device_id=at_offset(a, b), device_id_type=MESH)

    own = pl.ds(0, rows)
    small = (
        (p_h, xp0.at[own]), (r_h, xr0.at[own]), (cols_h, cols), (live_h, live), (needed_h, needed),
        (shifts_h, shifts), (diag_h, diag),
    )

    def small_copy(i):
        return pltpu.make_async_copy(small[i][0], small[i][1], in_sem.at[i])

    def chunk(c):
        part = (
            (slice(None), pl.ds(0, 1)),
            (pl.ds(0, MXU_ROWS), pl.ds(1, slots - 1)),
            (pl.ds(MXU_ROWS, rows - MXU_ROWS), pl.ds(1, slots - 1)),
        )[c]
        return pltpu.make_async_copy(a_h.at[part], a_v.at[part], a_sem.at[c])

    for i in range(len(small)):
        small_copy(i).start()
    for c in range(3):
        chunk(c).start()

    def copy(which, par, k, whole):
        if whole:
            src, size = xs[which][par].at[own], rows
        else:
            src, size = outbox.at[which, par, pl.ds(k * halo, halo)], halo
        return pltpu.make_async_remote_copy(
            src_ref=src,
            dst_ref=xs[which][par].at[pl.ds((1 + k) * rows, size)],
            send_sem=send_sem.at[which, par],
            recv_sem=recv_sem.at[which, par],
            device_id=peers[k],
            device_id_type=MESH,
        )

    def start(which, par, whole=False):
        for k in order:
            guarded(sends[k], lambda k=k: copy(which, par, k, whole).start())

    def halos(which, par, count):
        part = xs[which][par].at[pl.ds(rows, count)]
        return pltpu.make_async_remote_copy(
            src_ref=part, dst_ref=part, send_sem=send_sem.at[which, par], recv_sem=recv_sem.at[which, par],
            device_id=peers[2], device_id_type=MESH,
        )

    def both(x, y):
        return y if x is None else jnp.logical_and(x, y)

    def per_side(fn, whole, ok=None):
        for count, side in ((4, inner), (3, jnp.logical_not(inner))):
            if whole is None or whole is False:
                pl.when(both(ok, side))(lambda count=count: fn(count * halo))
            elif whole is True:
                pl.when(both(ok, side))(lambda count=count: fn(count * rows))
            else:
                pl.when(both(ok, jnp.logical_and(side, whole)))(lambda count=count: fn(count * rows))
                pl.when(both(ok, jnp.logical_and(side, jnp.logical_not(whole))))(lambda count=count: fn(count * halo))

    def wait_send(which, par, whole, ok=None):
        per_side(lambda size: halos(which, par, size).wait_send(), whole, ok)

    def wait_recv(which, par, whole):
        per_side(lambda size: halos(which, par, size).wait_recv(), whole)

    def list_copy(j):
        return pltpu.make_async_remote_copy(
            src_ref=needed, dst_ref=want.at[j], send_sem=l_send.at[j], recv_sem=l_recv.at[j],
            device_id=peers[j ^ 1], device_id_type=MESH,
        )

    asks = (m > 0, m < n_dom - 1, None, None)
    asked = sends

    fields[...] = jnp.zeros_like(fields)
    small_copy(0).wait()
    small_copy(1).wait()
    pl.semaphore_wait(barrier, n_group + inner.astype(jnp.int32) if near else n - 1)
    small_copy(4).wait()
    for j in range(4):
        guarded(asks[j], lambda j=j: list_copy(j).start())
    for which in range(2):
        start(which, 0, True)

    for i in (2, 3, 5, 6):
        small_copy(i).wait()
    wide = rows + 4 * halo
    for c in range(rows):
        spot[c] = c
        spot[wide + c] = c
    for k in range(4):
        for h in range(halo):
            spot[rows + k * halo + h] = (1 + k) * rows + needed[k, h]
            spot[wide + rows + k * halo + h] = (1 + k) * rows + h
    for b in range(rows):
        used = live[b]
        for s in range(1, slots):
            c = cols[s, b]
            idx[b * slots + s] = jnp.where(s < used, spot[c], zero_row)
            idx[(rows + b) * slots + s] = jnp.where(s < used, spot[wide + c], zero_row)

    for which in range(2):
        x = xs[which][0][own, :]
        basis[which * (depth + 1)] = x
        fields[:, which * (depth + 1), :] = x

    def folded(acc):
        return jnp.transpose(acc).reshape(bs // SUB, SUB, bs).sum(axis=0)

    def before(which, par, theta):
        x = xs[which][par]
        for q in range(groups):
            at = pl.ds(q * SUB, SUB)
            parts = [folded(a_v[q * SUB + i, 0] * x[pl.ds(q * SUB + i, 1), :]) for i in range(SUB)]
            y0[which, at, :] = jnp.stack(parts).sum(axis=1) + (diag[at, :] - theta) * x[at, :]

    def main(which, par, column, more, keep, base, first=None):
        x = xs[which][par]

        def row(b):
            acc = None
            for s in range(1, slots):
                term = a_v[b, s] * x[pl.ds(idx[base + b * slots + s], 1), :]
                acc = term if acc is None else acc + term
            return folded(acc)

        def finish(q, parts):
            at = pl.ds(q * SUB, SUB)
            y = jnp.stack(parts).sum(axis=1) + y0[which, at, :]
            if more:
                fresh[which, at, :] = y
                xs[which][1 - par][at, :] = y
            basis[column, at, :] = y
            if keep:
                fields[at, column, :] = y

        sub = lax.broadcasted_iota(jnp.int32, (SUB, bs), 0)

        def pair(p):
            acc = None
            for s in range(1, slots):
                v = jnp.where(
                    sub < 2,
                    x[pl.ds(idx[base + 2 * p * slots + s], 1), :],
                    x[pl.ds(idx[base + (2 * p + 1) * slots + s], 1), :],
                )
                hi = v.astype(jnp.bfloat16).astype(jnp.float32)
                lhs = jnp.where(sub % 2 == 0, hi, v - hi).astype(jnp.bfloat16)
                term = jnp.dot(
                    jnp.concatenate([lhs, lhs], axis=1), w_v[p, s - 1], preferred_element_type=jnp.float32
                )
                acc = term if acc is None else acc + term
            return [
                jnp.where(sub < 2, acc[:, :bs], 0.0),
                jnp.where(sub // 2 == 1, acc[:, bs:], 0.0),
            ]

        parts, born, done = {}, {}, set()

        def close(q):
            finish(q, [parts.pop(q * SUB + i) for i in range(SUB)])
            done.add(q)

        def settle(now, lag):
            for q in range(groups):
                mine = range(q * SUB, q * SUB + SUB)
                if q not in done and all(b in parts for b in mine) and now - max(born[b] for b in mine) >= lag:
                    close(q)

        pairs = list(range(MXU_ROWS // 2))
        todo = list(range(MXU_ROWS, rows))
        for i, b in enumerate(todo):
            while pairs and i >= 0.8 * len(todo) * (MXU_ROWS // 2 - len(pairs)) / (MXU_ROWS // 2):
                p = pairs.pop(0)
                parts[2 * p], parts[2 * p + 1] = pair(p)
                born[2 * p] = born[2 * p + 1] = i + 4
            parts[b] = row(b)
            born[b] = i
            settle(i, 4)
        settle(len(todo), -rows)
        if more:
            if first is not None and which == 0 and par == 0:
                for j in range(4):
                    pl.when(both(asked[j], first))(lambda j=j: list_copy(j).wait_recv())
                    pl.when(both(asks[j], first))(lambda j=j: list_copy(j).wait_send())
            for k in order:
                for h in range(halo):
                    outbox[which, 1 - par, pl.ds(k * halo + h, 1), :] = fresh[which, pl.ds(want[k, k, h], 1), :]
                guarded(sends[k], lambda k=k: copy(which, 1 - par, k, False).start())

    chunk(0).wait()
    before(0, 0, shifts[0])
    chunk(1).wait()

    def weights(p, carry):
        for s in range(1, slots):
            for e in range(2):
                t = jnp.transpose(a_v[2 * p + e, s])
                hi, lo = split(t)
                w_v[p, s - 1, pl.ds(0, bs), pl.ds(e * bs, bs)] = hi
                w_v[p, s - 1, pl.ds(bs, bs), pl.ds(e * bs, bs)] = lo
        return carry

    lax.fori_loop(0, MXU_ROWS // 2, weights, 0)
    chunk(2).wait()

    full = rows * slots

    def turn(which, k, par, more, first, keep=True):
        if which == 1:
            before(which, par, shifts[k - 1])
        if first is None:
            wait_recv(which, par, False)
            wait_send(which, 1 - par, False)
        elif par == 0:
            wait_recv(which, par, first)
            wait_send(which, 1 - par, False, jnp.logical_not(first))
        else:
            wait_recv(which, par, False)
            wait_send(which, 1 - par, first)
        base = jnp.where(first, 0, full) if first is not None and par == 0 else full
        main(which, par, which * (depth + 1) + k, more, keep, base, first)
        if more and which == 0:
            before(which, 1 - par, shifts[k])

    def two(t, carry):
        for par in range(2):
            for which in range(2):
                turn(which, 2 * t + 1 + par, par, True, t == 0)
        return carry

    trips = (depth - 2) // 2
    lax.fori_loop(0, trips, two, 0)
    for k in range(2 * trips + 1, depth - 1):
        for which in range(2):
            turn(which, k, (k - 1) % 2, which == 0 or k < depth - 1, None)

    def share(a, b, src, dst, i):
        return pltpu.make_async_remote_copy(
            src_ref=src, dst_ref=dst.at[me], send_sem=g_send.at[i], recv_sem=g_recv.at[i],
            device_id=at_offset(a, b), device_id_type=MESH,
        )

    def shared(dst, i):
        part = dst.at[pl.ds(0, n - 1)]
        return pltpu.make_async_remote_copy(
            src_ref=part, dst_ref=part, send_sem=g_send.at[i], recv_sem=g_recv.at[i],
            device_id=peers[2], device_id_type=MESH,
        )

    turn(0, depth - 1, depth % 2, True, None, False)
    acc = None
    for b in range(rows):
        hi, lo = split(fields[b])
        pair = jnp.concatenate([hi, lo], axis=0)
        term = lax.dot_general(pair, pair, (((1,), (1,)), ((), ())), preferred_element_type=jnp.float32)
        acc = term if acc is None else acc + term
    top = acc[:width] + acc[width:]
    part = top[:, :width] + top[:, width:]
    wide = jnp.concatenate([part, jnp.zeros((width, bs - width), jnp.float32)], axis=1)
    packed = wide[:SUB]
    for t in range(1, -(-count // SUB)):
        packed = packed + pltpu.roll(wide[t * SUB:(t + 1) * SUB], t * PACK, 1)
    g_own[...] = packed

    for a, b in others:
        share(a, b, g_own, g_all, 0).start()
    g_all[me] = g_own[...]
    turn(1, depth - 1, depth % 2, False, None, False)

    late = (depth - 1, 2 * depth, depth)

    def products(c, known):
        x = basis[c].reshape(groups, SUB, bs)
        sums = []
        for j in range(PACK):
            if j in known:
                sums.append((x * basis[j].reshape(groups, SUB, bs)).sum(axis=0))
            else:
                sums.append(jnp.zeros((SUB, bs), jnp.float32))
        return jnp.stack(sums).sum(axis=1)

    seen = [j for j in range(count) if j != depth]
    halves = [products(late[0], seen), products(late[1], seen)]
    early = jnp.transpose(jnp.concatenate(halves + [jnp.zeros((bs - 2 * PACK, bs), jnp.float32)], axis=0))
    early = early.sum(axis=0, keepdims=True)

    wait_recv(0, (depth - 1) % 2, False)
    main(0, (depth - 1) % 2, depth, False, False, full)
    pad = jnp.zeros((2 * PACK, bs), jnp.float32)
    end = jnp.concatenate([pad, products(depth, list(range(count))), pad[:bs - 3 * PACK]], axis=0)
    line = jnp.transpose(end).sum(axis=0, keepdims=True) + early
    row_own[...] = line
    for a, b in others:
        share(a, b, row_own, row_all, 1).start()
    row_all[me] = line

    shared(g_all, 0).wait_recv()
    total = g_all[...].sum(axis=0)
    pieces = [total] + [pltpu.roll(total, bs - t * PACK, 1) for t in range(1, -(-count // SUB))]
    table = jnp.concatenate(pieces, axis=0)
    r_id = lax.broadcasted_iota(jnp.int32, table.shape, 0)
    c_id = lax.broadcasted_iota(jnp.int32, table.shape, 1)
    shared(row_all, 1).wait_recv()
    sweep = jnp.broadcast_to(row_all[...].reshape(n, bs).sum(axis=0, keepdims=True), table.shape)
    for i in (1, 0, 2):
        c = late[i]
        across = sweep if i == 0 else pltpu.roll(sweep, bs - i * PACK, 1)
        down = jnp.where(c_id == r_id + i * PACK, sweep, 0.0).sum(axis=1, keepdims=True)
        table = jnp.where(r_id == c, across, jnp.where(c_id == c, down, table))
    gram[...] = table[:count, :count] * (1.0 / (n * rows * bs))

    wait_send(0, 0, False)
    wait_send(0, 1, False)
    wait_send(1, (depth - 2) % 2, False)
    shared(g_all, 0).wait_send()
    shared(row_all, 1).wait_send()


def export(b_ref, g_ref, b_out, g_out, sem):
    copies = [pltpu.make_async_copy(b_ref, b_out, sem.at[0]), pltpu.make_async_copy(g_ref, g_out, sem.at[1])]
    for c in copies:
        c.start()
    for c in copies:
        c.wait()


def per_device(n_group, n_dom, p_start, r_start, diag_shift, shifts, block_values, block_cols, live_slots, needed):
    rows, bs = p_start.shape
    slots = block_values.shape[1]
    depth = shifts.shape[0]
    halo = needed.shape[2]
    columns = 2 * depth + 1
    width = -(-columns // SUB) * SUB
    n = n_group * n_dom
    hbm = pl.BlockSpec(memory_space=pltpu.HBM)
    vmem = pl.BlockSpec(memory_space=pltpu.VMEM)
    ext = pltpu.VMEM((5 * rows + SUB, bs), jnp.float32)
    basis, gram = pl.pallas_call(
        functools.partial(kernel, n_group, n_dom),
        out_shape=(
            jax.ShapeDtypeStruct((columns, rows, bs), jnp.float32),
            jax.ShapeDtypeStruct((columns, columns), jnp.float32),
        ),
        in_specs=[hbm] * 8,
        out_specs=(vmem, vmem),
        scratch_shapes=[
            pltpu.SMEM((depth,), jnp.float32),
            pltpu.SMEM((slots, rows), jnp.int32),
            pltpu.SMEM((rows,), jnp.int32),
            pltpu.SMEM((4, halo), jnp.int32),
            pltpu.VMEM(block_values.shape, jnp.float32),
            pltpu.VMEM((MXU_ROWS // 2, slots - 1, 2 * bs, 2 * bs), jnp.bfloat16),
            ext, ext, ext, ext,
            pltpu.VMEM((2, rows, bs), jnp.float32),
            pltpu.VMEM((rows, bs), jnp.float32),
            pltpu.SMEM((2 * rows * slots,), jnp.int32),
            pltpu.SMEM((2 * (rows + 4 * halo),), jnp.int32),
            pltpu.SMEM((4, 4, halo), jnp.int32),
            pltpu.VMEM((2, rows, bs), jnp.float32),
            pltpu.VMEM((2, 2, 4 * halo, bs), jnp.float32),
            pltpu.VMEM((rows, width, bs), jnp.float32),
            pltpu.VMEM((SUB, bs), jnp.float32),
            pltpu.VMEM((n, SUB, bs), jnp.float32),
            pltpu.VMEM((1, bs), jnp.float32),
            pltpu.VMEM((n, 1, bs), jnp.float32),
            pltpu.SemaphoreType.DMA((7,)),
            pltpu.SemaphoreType.DMA((3,)),
            pltpu.SemaphoreType.DMA((2, 2)),
            pltpu.SemaphoreType.DMA((2, 2)),
            pltpu.SemaphoreType.DMA((2,)),
            pltpu.SemaphoreType.DMA((2,)),
            pltpu.SemaphoreType.DMA((4,)),
            pltpu.SemaphoreType.DMA((4,)),
        ],
        compiler_params=pltpu.CompilerParams(
            collective_id=0, has_side_effects=True, vmem_limit_bytes=24 * 1024 * 1024
        ),
    )(*[pltpu.with_memory_space_constraint(v, pltpu.HBM) for v in (
        shifts, block_cols.T, live_slots, needed[0], p_start, r_start, diag_shift, block_values)])
    return pl.pallas_call(
        export,
        out_shape=(
            jax.ShapeDtypeStruct(basis.shape, jnp.float32),
            jax.ShapeDtypeStruct(gram.shape, jnp.float32),
        ),
        in_specs=[vmem, vmem],
        out_specs=(hbm, hbm),
        scratch_shapes=[pltpu.SemaphoreType.DMA((2,))],
        compiler_params=pltpu.CompilerParams(vmem_limit_bytes=4 * 1024 * 1024),
    )(basis, gram)


def solution(mesh):
    return jax.shard_map(
        functools.partial(per_device, mesh.shape["group"], mesh.shape["dom"]),
        mesh=mesh,
        in_specs=(
            P(("group", "dom"), None),
            P(("group", "dom"), None),
            P(("group", "dom"), None),
            P(),
            P(("group", "dom"), None, None, None),
            P(("group", "dom"), None),
            P(("group", "dom")),
            P(("group", "dom"), None, None),
        ),
        out_specs=(P(None, ("group", "dom"), None), P()),
        check_vma=False,
    )
```

```python
import functools

import jax
import jax.numpy as jnp
from jax import lax
from jax.experimental import pallas as pl
from jax.experimental.pallas import tpu as pltpu
from jax.sharding import PartitionSpec as P

MESH = pl.DeviceIdType.MESH
SUB = 8
PACK = 32
MXU_ROWS = 8


def split(x):
    hi = x.astype(jnp.bfloat16)
    lo = (x - hi.astype(jnp.float32)).astype(jnp.bfloat16)
    return hi, lo


def kernel(n_group, n_dom, shifts_h, cols_h, live_h, needed_h, p_h, r_h, diag_h, a_h, basis, gram,
           shifts, cols, live, needed, a_v, w_v, xp0, xp1, xr0, xr1, y0, diag, idx, spot, want, fresh, outbox, fields, g_own, g_all, row_own, row_all,
           in_sem, a_sem, send_sem, recv_sem, g_send, g_recv, l_send, l_recv):
    rows, slots, bs, _ = a_v.shape
    depth = shifts.shape[0]
    halo = needed.shape[1]
    count = basis.shape[0]
    width = fields.shape[1]
    groups = rows // SUB
    zero_row = 5 * rows
    n = n_group * n_dom
    g, m = lax.axis_index("group"), lax.axis_index("dom")
    me = g * n_dom + m

    xs = ((xp0, xp1), (xr0, xr1))
    for which in range(2):
        for par in range(2):
            xs[which][par][pl.ds(rows, 2 * rows), :] = jnp.zeros((2 * rows, bs), jnp.float32)
            xs[which][par][pl.ds(zero_row, SUB), :] = jnp.zeros((SUB, bs), jnp.float32)

    for k in range(2):
        for h in range(halo):
            want[k, k, h] = 0

    peers = (
        (g, lax.rem(m + 1, n_dom)),
        (g, lax.rem(m + n_dom - 1, n_dom)),
        (lax.rem(g + 1, n_group), m),
        (lax.rem(g + n_group - 1, n_group), m),
    )
    sends = (m < n_dom - 1, m > 0, None, None)
    order = (2, 3, 0, 1)
    inner = jnp.logical_and(m > 0, m < n_dom - 1)
    others = [(a, b) for b in range(n_dom) for a in range(n_group) if a + b > 0]
    others.sort(key=lambda o: (o[1] == 0, o[1], -abs(o[0] - n_group / 2 + 0.5)))

    def at_offset(a, b):
        return lax.rem(g + a, n_group), lax.rem(m + b, n_dom)

    def guarded(ok, fn):
        if ok is None:
            fn()
        else:
            pl.when(ok)(fn)

    barrier = pltpu.get_barrier_semaphore()
    near = n_dom <= depth
    if near:
        for a in range(1, n_group):
            pl.semaphore_signal(barrier, inc=1, device_id=at_offset(a, 0), device_id_type=MESH)
        for k in (0, 1):
            guarded(sends[k], lambda k=k: pl.semaphore_signal(
                barrier, inc=1, device_id=peers[k], device_id_type=MESH))
    else:
        for a, b in others:
            pl.semaphore_signal(barrier, inc=1, device_id=at_offset(a, b), device_id_type=MESH)

    own = pl.ds(0, rows)
    small = (
        (p_h, xp0.at[own]), (r_h, xr0.at[own]), (cols_h, cols), (live_h, live), (needed_h, needed),
        (shifts_h, shifts), (diag_h, diag),
    )

    def small_copy(i):
        return pltpu.make_async_copy(small[i][0], small[i][1], in_sem.at[i])

    def chunk(c):
        part = (
            (slice(None), pl.ds(0, 1)),
            (pl.ds(0, MXU_ROWS), pl.ds(1, slots - 1)),
            (pl.ds(MXU_ROWS, rows - MXU_ROWS), pl.ds(1, slots - 1)),
        )[c]
        return pltpu.make_async_copy(a_h.at[part], a_v.at[part], a_sem.at[c])

    for i in range(len(small)):
        small_copy(i).start()
    for c in range(3):
        chunk(c).start()

    def copy(which, par, k, whole):
        if whole:
            src, size = xs[which][par].at[own], rows
        else:
            src, size = outbox.at[which, par, pl.ds(k * halo, halo)], halo
        return pltpu.make_async_remote_copy(
            src_ref=src,
            dst_ref=xs[which][par].at[pl.ds((1 + k) * rows, size)],
            send_sem=send_sem.at[which, par],
            recv_sem=recv_sem.at[which, par],
            device_id=peers[k],
            device_id_type=MESH,
        )

    def start(which, par, whole=False):
        for k in order:
            guarded(sends[k], lambda k=k: copy(which, par, k, whole).start())

    def halos(which, par, count):
        part = xs[which][par].at[pl.ds(rows, count)]
        return pltpu.make_async_remote_copy(
            src_ref=part, dst_ref=part, send_sem=send_sem.at[which, par], recv_sem=recv_sem.at[which, par],
            device_id=peers[2], device_id_type=MESH,
        )

    def both(x, y):
        return y if x is None else jnp.logical_and(x, y)

    def per_side(fn, whole, ok=None):
        for count, side in ((4, inner), (3, jnp.logical_not(inner))):
            if whole is None or whole is False:
                pl.when(both(ok, side))(lambda count=count: fn(count * halo))
            elif whole is True:
                pl.when(both(ok, side))(lambda count=count: fn(count * rows))
            else:
                pl.when(both(ok, jnp.logical_and(side, whole)))(lambda count=count: fn(count * rows))
                pl.when(both(ok, jnp.logical_and(side, jnp.logical_not(whole))))(lambda count=count: fn(count * halo))

    def wait_send(which, par, whole, ok=None):
        per_side(lambda size: halos(which, par, size).wait_send(), whole, ok)

    def wait_recv(which, par, whole):
        per_side(lambda size: halos(which, par, size).wait_recv(), whole)

    def list_copy(j):
        return pltpu.make_async_remote_copy(
            src_ref=needed, dst_ref=want.at[j], send_sem=l_send.at[j], recv_sem=l_recv.at[j],
            device_id=peers[j ^ 1], device_id_type=MESH,
        )

    asks = (m > 0, m < n_dom - 1, None, None)
    asked = sends

    small_copy(0).wait()
    small_copy(1).wait()
    pl.semaphore_wait(barrier, n_group + inner.astype(jnp.int32) if near else n - 1)
    small_copy(4).wait()
    for j in range(4):
        guarded(asks[j], lambda j=j: list_copy(j).start())
    for which in range(2):
        start(which, 0, True)

    for i in (2, 3, 5, 6):
        small_copy(i).wait()
    wide = rows + 4 * halo
    for c in range(rows):
        spot[c] = c
        spot[wide + c] = c
    for k in range(4):
        for h in range(halo):
            spot[rows + k * halo + h] = (1 + k) * rows + needed[k, h]
            spot[wide + rows + k * halo + h] = (1 + k) * rows + h
    for b in range(rows):
        used = live[b]
        for s in range(1, slots):
            c = cols[s, b]
            idx[b * slots + s] = jnp.where(s < used, spot[c], zero_row)
            idx[(rows + b) * slots + s] = jnp.where(s < used, spot[wide + c], zero_row)

    fields[...] = jnp.zeros_like(fields)
    for which in range(2):
        x = xs[which][0][own, :]
        basis[which * (depth + 1)] = x
        fields[:, which * (depth + 1), :] = x

    def folded(acc):
        return jnp.transpose(acc).reshape(bs // SUB, SUB, bs).sum(axis=0)

    def before(which, par, theta):
        x = xs[which][par]
        for q in range(groups):
            at = pl.ds(q * SUB, SUB)
            parts = [folded(a_v[q * SUB + i, 0] * x[pl.ds(q * SUB + i, 1), :]) for i in range(SUB)]
            y0[which, at, :] = jnp.stack(parts).sum(axis=1) + (diag[at, :] - theta) * x[at, :]

    def main(which, par, column, more, keep, base, first=None):
        x = xs[which][par]

        def row(b):
            acc = None
            for s in range(1, slots):
                term = a_v[b, s] * x[pl.ds(idx[base + b * slots + s], 1), :]
                acc = term if acc is None else acc + term
            return folded(acc)

        def finish(q, parts):
            at = pl.ds(q * SUB, SUB)
            y = jnp.stack(parts).sum(axis=1) + y0[which, at, :]
            if more:
                fresh[which, at, :] = y
                xs[which][1 - par][at, :] = y
            basis[column, at, :] = y
            if keep:
                fields[at, column, :] = y

        sub = lax.broadcasted_iota(jnp.int32, (SUB, bs), 0)

        def pair(p):
            acc = None
            for s in range(1, slots):
                v = jnp.where(
                    sub < 2,
                    x[pl.ds(idx[base + 2 * p * slots + s], 1), :],
                    x[pl.ds(idx[base + (2 * p + 1) * slots + s], 1), :],
                )
                hi = v.astype(jnp.bfloat16).astype(jnp.float32)
                lhs = jnp.where(sub % 2 == 0, hi, v - hi).astype(jnp.bfloat16)
                term = jnp.dot(
                    jnp.concatenate([lhs, lhs], axis=1), w_v[p, s - 1], preferred_element_type=jnp.float32
                )
                acc = term if acc is None else acc + term
            return [
                jnp.where(sub < 2, acc[:, :bs], 0.0),
                jnp.where(sub // 2 == 1, acc[:, bs:], 0.0),
            ]

        parts, born, done = {}, {}, set()

        def close(q):
            finish(q, [parts.pop(q * SUB + i) for i in range(SUB)])
            done.add(q)

        def settle(now, lag):
            for q in range(groups):
                mine = range(q * SUB, q * SUB + SUB)
                if q not in done and all(b in parts for b in mine) and now - max(born[b] for b in mine) >= lag:
                    close(q)

        pairs = list(range(MXU_ROWS // 2))
        todo = list(range(MXU_ROWS, rows))
        for i, b in enumerate(todo):
            while pairs and i >= 0.8 * len(todo) * (MXU_ROWS // 2 - len(pairs)) / (MXU_ROWS // 2):
                p = pairs.pop(0)
                parts[2 * p], parts[2 * p + 1] = pair(p)
                born[2 * p] = born[2 * p + 1] = i + 4
            parts[b] = row(b)
            born[b] = i
            settle(i, 4)
        settle(len(todo), -rows)
        if more:
            if first is not None and which == 0 and par == 0:
                for j in range(4):
                    pl.when(both(asked[j], first))(lambda j=j: list_copy(j).wait_recv())
                    pl.when(both(asks[j], first))(lambda j=j: list_copy(j).wait_send())
            for k in order:
                for h in range(halo):
                    outbox[which, 1 - par, pl.ds(k * halo + h, 1), :] = fresh[which, pl.ds(want[k, k, h], 1), :]
                guarded(sends[k], lambda k=k: copy(which, 1 - par, k, False).start())

    chunk(0).wait()
    before(0, 0, shifts[0])
    chunk(1).wait()

    def weights(p, carry):
        for s in range(1, slots):
            for e in range(2):
                t = jnp.transpose(a_v[2 * p + e, s])
                hi, lo = split(t)
                w_v[p, s - 1, pl.ds(0, bs), pl.ds(e * bs, bs)] = hi
                w_v[p, s - 1, pl.ds(bs, bs), pl.ds(e * bs, bs)] = lo
        return carry

    lax.fori_loop(0, MXU_ROWS // 2, weights, 0)
    chunk(2).wait()

    full = rows * slots

    def turn(which, k, par, more, first, keep=True):
        if which == 1:
            before(which, par, shifts[k - 1])
        if first is None:
            wait_recv(which, par, False)
            wait_send(which, 1 - par, False)
        elif par == 0:
            wait_recv(which, par, first)
            wait_send(which, 1 - par, False, jnp.logical_not(first))
        else:
            wait_recv(which, par, False)
            wait_send(which, 1 - par, first)
        base = jnp.where(first, 0, full) if first is not None and par == 0 else full
        main(which, par, which * (depth + 1) + k, more, keep, base, first)
        if more and which == 0:
            before(which, 1 - par, shifts[k])

    def two(t, carry):
        for par in range(2):
            for which in range(2):
                turn(which, 2 * t + 1 + par, par, True, t == 0)
        return carry

    trips = (depth - 2) // 2
    lax.fori_loop(0, trips, two, 0)
    for k in range(2 * trips + 1, depth - 1):
        for which in range(2):
            turn(which, k, (k - 1) % 2, which == 0 or k < depth - 1, None)

    def share(a, b, src, dst, i):
        return pltpu.make_async_remote_copy(
            src_ref=src, dst_ref=dst.at[me], send_sem=g_send.at[i], recv_sem=g_recv.at[i],
            device_id=at_offset(a, b), device_id_type=MESH,
        )

    def shared(dst, i):
        part = dst.at[pl.ds(0, n - 1)]
        return pltpu.make_async_remote_copy(
            src_ref=part, dst_ref=part, send_sem=g_send.at[i], recv_sem=g_recv.at[i],
            device_id=peers[2], device_id_type=MESH,
        )

    turn(0, depth - 1, depth % 2, True, None, False)
    acc = None
    for b in range(rows):
        hi, lo = split(fields[b])
        pair = jnp.concatenate([hi, lo], axis=0)
        term = lax.dot_general(pair, pair, (((1,), (1,)), ((), ())), preferred_element_type=jnp.float32)
        acc = term if acc is None else acc + term
    top = acc[:width] + acc[width:]
    part = top[:, :width] + top[:, width:]
    wide = jnp.concatenate([part, jnp.zeros((width, bs - width), jnp.float32)], axis=1)
    packed = wide[:SUB]
    for t in range(1, -(-count // SUB)):
        packed = packed + pltpu.roll(wide[t * SUB:(t + 1) * SUB], t * PACK, 1)
    g_own[...] = packed

    for a, b in others:
        share(a, b, g_own, g_all, 0).start()
    g_all[me] = g_own[...]
    turn(1, depth - 1, depth % 2, False, None, False)

    late = (depth - 1, 2 * depth, depth)

    def products(c, known):
        x = basis[c].reshape(groups, SUB, bs)
        sums = []
        for j in range(PACK):
            if j in known:
                sums.append((x * basis[j].reshape(groups, SUB, bs)).sum(axis=0))
            else:
                sums.append(jnp.zeros((SUB, bs), jnp.float32))
        return jnp.stack(sums).sum(axis=1)

    seen = [j for j in range(count) if j != depth]
    halves = [products(late[0], seen), products(late[1], seen)]
    early = jnp.transpose(jnp.concatenate(halves + [jnp.zeros((bs - 2 * PACK, bs), jnp.float32)], axis=0))
    early = early.sum(axis=0, keepdims=True)

    wait_recv(0, (depth - 1) % 2, False)
    main(0, (depth - 1) % 2, depth, False, False, full)
    pad = jnp.zeros((2 * PACK, bs), jnp.float32)
    end = jnp.concatenate([pad, products(depth, list(range(count))), pad[:bs - 3 * PACK]], axis=0)
    line = jnp.transpose(end).sum(axis=0, keepdims=True) + early
    row_own[...] = line
    for a, b in others:
        share(a, b, row_own, row_all, 1).start()
    row_all[me] = line

    shared(g_all, 0).wait_recv()
    total = g_all[...].sum(axis=0)
    pieces = [total] + [pltpu.roll(total, bs - t * PACK, 1) for t in range(1, -(-count // SUB))]
    table = jnp.concatenate(pieces, axis=0)
    r_id = lax.broadcasted_iota(jnp.int32, table.shape, 0)
    c_id = lax.broadcasted_iota(jnp.int32, table.shape, 1)
    shared(row_all, 1).wait_recv()
    sweep = jnp.broadcast_to(row_all[...].reshape(n, bs).sum(axis=0, keepdims=True), table.shape)
    for i in (1, 0, 2):
        c = late[i]
        across = sweep if i == 0 else pltpu.roll(sweep, bs - i * PACK, 1)
        down = jnp.where(c_id == r_id + i * PACK, sweep, 0.0).sum(axis=1, keepdims=True)
        table = jnp.where(r_id == c, across, jnp.where(c_id == c, down, table))
    gram[...] = table[:count, :count] * (1.0 / (n * rows * bs))

    wait_send(0, 0, False)
    wait_send(0, 1, False)
    wait_send(1, (depth - 2) % 2, False)
    shared(g_all, 0).wait_send()
    shared(row_all, 1).wait_send()


def export(b_ref, g_ref, b_out, g_out, sem):
    copies = [pltpu.make_async_copy(b_ref, b_out, sem.at[0]), pltpu.make_async_copy(g_ref, g_out, sem.at[1])]
    for c in copies:
        c.start()
    for c in copies:
        c.wait()


def per_device(n_group, n_dom, p_start, r_start, diag_shift, shifts, block_values, block_cols, live_slots, needed):
    rows, bs = p_start.shape
    slots = block_values.shape[1]
    depth = shifts.shape[0]
    halo = needed.shape[2]
    columns = 2 * depth + 1
    width = -(-columns // SUB) * SUB
    n = n_group * n_dom
    hbm = pl.BlockSpec(memory_space=pltpu.HBM)
    vmem = pl.BlockSpec(memory_space=pltpu.VMEM)
    ext = pltpu.VMEM((5 * rows + SUB, bs), jnp.float32)
    basis, gram = pl.pallas_call(
        functools.partial(kernel, n_group, n_dom),
        out_shape=(
            jax.ShapeDtypeStruct((columns, rows, bs), jnp.float32),
            jax.ShapeDtypeStruct((columns, columns), jnp.float32),
        ),
        in_specs=[hbm] * 8,
        out_specs=(vmem, vmem),
        scratch_shapes=[
            pltpu.SMEM((depth,), jnp.float32),
            pltpu.SMEM((slots, rows), jnp.int32),
            pltpu.SMEM((rows,), jnp.int32),
            pltpu.SMEM((4, halo), jnp.int32),
            pltpu.VMEM(block_values.shape, jnp.float32),
            pltpu.VMEM((MXU_ROWS // 2, slots - 1, 2 * bs, 2 * bs), jnp.bfloat16),
            ext, ext, ext, ext,
            pltpu.VMEM((2, rows, bs), jnp.float32),
            pltpu.VMEM((rows, bs), jnp.float32),
            pltpu.SMEM((2 * rows * slots,), jnp.int32),
            pltpu.SMEM((2 * (rows + 4 * halo),), jnp.int32),
            pltpu.SMEM((4, 4, halo), jnp.int32),
            pltpu.VMEM((2, rows, bs), jnp.float32),
            pltpu.VMEM((2, 2, 4 * halo, bs), jnp.float32),
            pltpu.VMEM((rows, width, bs), jnp.float32),
            pltpu.VMEM((SUB, bs), jnp.float32),
            pltpu.VMEM((n, SUB, bs), jnp.float32),
            pltpu.VMEM((1, bs), jnp.float32),
            pltpu.VMEM((n, 1, bs), jnp.float32),
            pltpu.SemaphoreType.DMA((7,)),
            pltpu.SemaphoreType.DMA((3,)),
            pltpu.SemaphoreType.DMA((2, 2)),
            pltpu.SemaphoreType.DMA((2, 2)),
            pltpu.SemaphoreType.DMA((2,)),
            pltpu.SemaphoreType.DMA((2,)),
            pltpu.SemaphoreType.DMA((4,)),
            pltpu.SemaphoreType.DMA((4,)),
        ],
        compiler_params=pltpu.CompilerParams(
            collective_id=0, has_side_effects=True, vmem_limit_bytes=24 * 1024 * 1024,
        ),
    )(*[pltpu.with_memory_space_constraint(v, pltpu.HBM) for v in (
        shifts, block_cols.T, live_slots, needed[0], p_start, r_start, diag_shift, block_values)])
    return pl.pallas_call(
        export,
        out_shape=(
            jax.ShapeDtypeStruct(basis.shape, jnp.float32),
            jax.ShapeDtypeStruct(gram.shape, jnp.float32),
        ),
        in_specs=[vmem, vmem],
        out_specs=(hbm, hbm),
        scratch_shapes=[pltpu.SemaphoreType.DMA((2,))],
        compiler_params=pltpu.CompilerParams(vmem_limit_bytes=4 * 1024 * 1024),
    )(basis, gram)


def solution(mesh):
    return jax.shard_map(
        functools.partial(per_device, mesh.shape["group"], mesh.shape["dom"]),
        mesh=mesh,
        in_specs=(
            P(("group", "dom"), None),
            P(("group", "dom"), None),
            P(("group", "dom"), None),
            P(),
            P(("group", "dom"), None, None, None),
            P(("group", "dom"), None),
            P(("group", "dom")),
            P(("group", "dom"), None, None),
        ),
        out_specs=(P(None, ("group", "dom"), None), P()),
        check_vma=False,
    )
```
